16 devices in a mesh: dp: 2 (over y, z), cp: 8 (over x, core).
Axes of the slice: x: 4, y: 2, z: 1, core: 2. Of those that a mesh axis runs over, the one named last changes fastest.
The devices are a block of a 4x4x8 slice.
Arguments:
- q_raw: bfloat16 [16384, 16, 128], P(('dp', 'cp')), parts along dimension 0
- k_raw: bfloat16 [16384, 8, 128], P(('dp', 'cp')), parts along dimension 0
- v_proj: bfloat16 [16384, 8, 128], P(('dp', 'cp')), parts along dimension 0
- out_fwd: bfloat16 [16384, 16, 128], P(('dp', 'cp')), parts along dimension 0
- lse_fwd: float32 [16384, 16], P(('dp', 'cp')), parts along dimension 0
- d_out: bfloat16 [16384, 16, 128], P(('dp', 'cp')), parts along dimension 0
- q_norm: float32 [128], replicated
- k_norm: float32 [128], replicated
Outputs:
- output 1: bfloat16 [16384, 16, 128], P(('dp', 'cp')), parts along dimension 0
- output 2: bfloat16 [16384, 8, 128], P(('dp', 'cp')), parts along dimension 0
- output 3: bfloat16 [16384, 8, 128], P(('dp', 'cp')), parts along dimension 0
- output 4: float32 [256], P('dp'), parts along dimension 0
- output 5: float32 [256], P('dp'), parts along dimension 0
There are 2 independent parts. The reference program is written for one: setup_inputs(seed, part) draws one part's arguments, and reference() takes and returns one part's arrays. A program takes and returns all parts, laid end to end along the dimension named above; an argument that names none is the same for every part.
All inputs are finite; a program needn't handle non-finite values.
Results may differ from the reference program's by a relative error of at most 0.00316113.
Values are sent between devices in bfloat16 or wider.
A program may use at most 768 MiB of HBM per device.

```python
import jax
import jax.numpy as jnp
from jax import lax

HEADS = 16
KV_HEADS = 8
HEAD_DIM = 128
CHUNK = 512
CP_RANKS = 8
QUERY_BLOCK = 64
SEQ_LEN = 2 * CP_RANKS * CHUNK
Q_PER_KV = HEADS // KV_HEADS
BLOCK_COUNT = SEQ_LEN // QUERY_BLOCK
ROPE_THETA = 1000000.0
NORM_EPS = 1e-6


def layout_positions():
    row_ids = jnp.arange(SEQ_LEN)
    owner_dev = row_ids // (2 * CHUNK)
    within = row_ids % (2 * CHUNK)
    chunk_id = jnp.where(within < CHUNK, owner_dev, 2 * CP_RANKS - 1 - owner_dev)
    return chunk_id * CHUNK + within % CHUNK


def rope_tables(positions):
    inv_freq = ROPE_THETA ** (-jnp.arange(0, HEAD_DIM, 2).astype(jnp.float32) / HEAD_DIM)
    angles = positions.astype(jnp.float32)[:, None] * inv_freq[None, :]
    angles = jnp.concatenate([angles, angles], axis=-1)
    return jnp.cos(angles)[:, None, :], jnp.sin(angles)[:, None, :]


def norm_rope(raw_in, weight, cos_t, sin_t):
    mean_sq = jnp.mean(raw_in * raw_in, axis=-1, keepdims=True)
    normed = raw_in * lax.rsqrt(mean_sq + NORM_EPS) * weight
    half_dim = raw_in.shape[-1] // 2
    rotated = jnp.concatenate([-normed[..., half_dim:], normed[..., :half_dim]], axis=-1)
    return normed * cos_t + rotated * sin_t


def forward_stats(q_raw, k_raw, v_proj, q_norm, k_norm):
    positions = layout_positions()
    cos_t, sin_t = rope_tables(positions)
    q_b = norm_rope(q_raw.astype(jnp.float32), q_norm, cos_t, sin_t).astype(jnp.bfloat16)
    k_b = norm_rope(k_raw.astype(jnp.float32), k_norm, cos_t, sin_t).astype(jnp.bfloat16)
    q_f = q_b.astype(jnp.float32).reshape(BLOCK_COUNT, QUERY_BLOCK, KV_HEADS, Q_PER_KV, HEAD_DIM)
    k_f = k_b.astype(jnp.float32)
    v_f = v_proj.astype(jnp.float32)
    sm_scale = HEAD_DIM ** -0.5

    def one_block(scan_in):
        q_blk, q_pos = scan_in
        logits = jnp.einsum('qngd,knd->qngk', q_blk, k_f) * sm_scale
        visible = (q_pos[:, None] >= positions[None, :])[:, None, None, :]
        logits = jnp.where(visible, logits, -jnp.inf)
        row_max = jnp.max(logits, axis=-1, keepdims=True)
        weights = jnp.exp(logits - row_max)
        row_sum = jnp.sum(weights, axis=-1, keepdims=True)
        out_blk = jnp.einsum('qngk,knd->qngd', weights / row_sum, v_f)
        lse_blk = (row_max + jnp.log(row_sum))[..., 0]
        return out_blk, lse_blk

    out_blocks, lse_blocks = lax.map(one_block, (q_f, positions.reshape(BLOCK_COUNT, QUERY_BLOCK)))
    out_fwd = out_blocks.reshape(SEQ_LEN, HEADS, HEAD_DIM).astype(jnp.bfloat16)
    return out_fwd, lse_blocks.reshape(SEQ_LEN, HEADS)


def setup_inputs(seed: int = 0, part: int = 0) -> dict:
    base_key = jax.random.key(seed)
    shared_key, part_key = jax.random.split(base_key)
    part_key = jax.random.fold_in(part_key, part)
    part_keys = jax.random.split(part_key, 4)
    shared_keys = jax.random.split(shared_key, 2)
    q_raw = jax.random.normal(part_keys[0], (SEQ_LEN, HEADS, HEAD_DIM), jnp.float32).astype(jnp.bfloat16)
    k_raw = jax.random.normal(part_keys[1], (SEQ_LEN, KV_HEADS, HEAD_DIM), jnp.float32).astype(jnp.bfloat16)
    v_proj = jax.random.normal(part_keys[2], (SEQ_LEN, KV_HEADS, HEAD_DIM), jnp.float32).astype(jnp.bfloat16)
    d_out = jax.random.normal(part_keys[3], (SEQ_LEN, HEADS, HEAD_DIM), jnp.float32).astype(jnp.bfloat16)
    q_norm = jax.random.uniform(shared_keys[0], (HEAD_DIM,), jnp.float32, minval=0.5, maxval=1.6)
    k_norm = jax.random.uniform(shared_keys[1], (HEAD_DIM,), jnp.float32, minval=0.5, maxval=1.6)
    out_fwd, lse_fwd = forward_stats(q_raw, k_raw, v_proj, q_norm, k_norm)
    return {'q_raw': q_raw, 'k_raw': k_raw, 'v_proj': v_proj, 'out_fwd': out_fwd, 'lse_fwd': lse_fwd, 'd_out': d_out, 'q_norm': q_norm, 'k_norm': k_norm}


def reference(q_raw, k_raw, v_proj, out_fwd, lse_fwd, d_out, q_norm, k_norm):
    positions = layout_positions()
    cos_t, sin_t = rope_tables(positions)
    q_full, pull_q = jax.vjp(lambda raw_in, weight: norm_rope(raw_in, weight, cos_t, sin_t), q_raw.astype(jnp.float32), q_norm)
    k_full, pull_k = jax.vjp(lambda raw_in, weight: norm_rope(raw_in, weight, cos_t, sin_t), k_raw.astype(jnp.float32), k_norm)
    q_f = q_full.astype(jnp.bfloat16).astype(jnp.float32)
    k_f = k_full.astype(jnp.bfloat16).astype(jnp.float32)
    v_f = v_proj.astype(jnp.float32)
    do_f = d_out.astype(jnp.float32)
    delta_sum = jnp.sum(do_f * out_fwd.astype(jnp.float32), axis=-1)
    sm_scale = HEAD_DIM ** -0.5
    scan_in = (q_f.reshape(BLOCK_COUNT, QUERY_BLOCK, KV_HEADS, Q_PER_KV, HEAD_DIM),
               do_f.reshape(BLOCK_COUNT, QUERY_BLOCK, KV_HEADS, Q_PER_KV, HEAD_DIM),
               lse_fwd.reshape(BLOCK_COUNT, QUERY_BLOCK, KV_HEADS, Q_PER_KV),
               delta_sum.reshape(BLOCK_COUNT, QUERY_BLOCK, KV_HEADS, Q_PER_KV),
               positions.reshape(BLOCK_COUNT, QUERY_BLOCK))

    def scan_step(loop_state, block_in):
        dk_acc, dv_acc = loop_state
        q_blk, do_blk, lse_blk, delta_blk, q_pos = block_in
        logits = jnp.einsum('qngd,knd->qngk', q_blk, k_f) * sm_scale - lse_blk[..., None]
        visible = (q_pos[:, None] >= positions[None, :])[:, None, None, :]
        attn_prob = jnp.exp(jnp.where(visible, logits, -jnp.inf))
        attn_dprob = jnp.einsum('qngd,knd->qngk', do_blk, v_f)
        score_grad = (attn_prob * (attn_dprob - delta_blk[..., None])).astype(jnp.bfloat16).astype(jnp.float32)
        prob_bf = attn_prob.astype(jnp.bfloat16).astype(jnp.float32)
        dq_blk = sm_scale * jnp.einsum('qngk,knd->qngd', score_grad, k_f)
        dk_acc = dk_acc + sm_scale * jnp.einsum('qngk,qngd->knd', score_grad, q_blk)
        dv_acc = dv_acc + jnp.einsum('qngk,qngd->knd', prob_bf, do_blk)
        return (dk_acc, dv_acc), dq_blk

    zero_kv = jnp.zeros((SEQ_LEN, KV_HEADS, HEAD_DIM), jnp.float32)
    (dk_sum, dv_sum), dq_blocks = lax.scan(scan_step, (zero_kv, zero_kv), scan_in)
    dq_raw, dq_norm = pull_q(dq_blocks.reshape(SEQ_LEN, HEADS, HEAD_DIM))
    dk_raw, dk_norm = pull_k(dk_sum)
    return (dq_raw.astype(jnp.bfloat16), dk_raw.astype(jnp.bfloat16), dv_sum.astype(jnp.bfloat16), dq_norm, dk_norm)
```

```python
import functools

import jax
import jax.numpy as jnp
from jax import lax
from jax.experimental import pallas as pl
from jax.experimental.pallas import tpu as pltpu
from jax.sharding import PartitionSpec as P

HEAD_DIM = 128
ROPE_THETA = 1000000.0
NORM_EPS = 1e-6
SM_SCALE = HEAD_DIM ** -0.5
F32 = jnp.float32
BF16 = jnp.bfloat16


def angle_tables(positions):
    inv_freq = ROPE_THETA ** (-jnp.arange(0, HEAD_DIM, 2).astype(F32) / HEAD_DIM)
    angles = positions.astype(F32)[:, None] * inv_freq[None, :]
    angles = jnp.concatenate([angles, angles], axis=-1)
    return jnp.cos(angles), jnp.sin(angles)


def lane_sign():
    lane = lax.broadcasted_iota(jnp.int32, (1, HEAD_DIM), 1)
    return jnp.where(lane < HEAD_DIM // 2, -1.0, 1.0).astype(F32)


def chunk_angles(c, cos_o, sin_o, cos_c, sin_c):
    cc, sc = cos_c[pl.ds(c, 1), :], sin_c[pl.ds(c, 1), :]
    co, so = cos_o[...], sin_o[...]
    return cc * co - sc * so, (sc * co + cc * so) * lane_sign()


def norm_rope(x, weight, cos_t, sin_s):
    rinv = lax.rsqrt(jnp.mean(x * x, axis=-1, keepdims=True) + NORM_EPS)
    y = x * rinv * weight
    return y * cos_t + pltpu.roll(y, HEAD_DIM // 2, 1) * sin_s


def norm_rope_grad(x, weight, cos_t, sin_s, g):
    rinv = lax.rsqrt(jnp.mean(x * x, axis=-1, keepdims=True) + NORM_EPS)
    n = x * rinv
    dy = g * cos_t + pltpu.roll(g * sin_s, HEAD_DIM // 2, 1)
    dw = dy * n
    dn = dy * weight
    dx = rinv * (dn - n * jnp.mean(dn * n, axis=-1, keepdims=True))
    return dx, jnp.sum(dw.reshape(-1, 8, HEAD_DIM), axis=0)


def split3(x):
    hi = x.astype(BF16).astype(F32)
    mid = (x - hi).astype(BF16).astype(F32)
    return hi, mid, x - hi - mid


def prep_chunk(c, raw, ld, qw, kw, tabs, qr, qt, dot_, ext):
    cos_t, sin_s = chunk_angles(c, *tabs)
    rows = raw.shape[1]
    for h in range(2):
        y = norm_rope(raw[c, :, h * 128:(h + 1) * 128].astype(F32), qw[...], cos_t, sin_s)
        qr[c, :, h * 128:(h + 1) * 128] = y.astype(BF16)
        qt[c, :, h * rows:(h + 1) * rows] = y.T.astype(BF16)
        dot_[c, :, h * rows:(h + 1) * rows] = raw[c, :, 512 + h * 128:640 + h * 128].astype(F32).T.astype(BF16)
    y = norm_rope(raw[c, :, 256:384].astype(F32), kw[...], cos_t, sin_s)
    qr[c, :, 256:384] = y.astype(BF16)
    vals = ld[c]
    parts = []
    for t in range(4):
        parts.extend(split3(vals[t:t + 1] * (1.0 / SM_SCALE if t < 2 else 1.0)))
    parts.append(jnp.zeros((HEAD_DIM - 12, rows), F32))
    ext[c] = jnp.concatenate(parts, axis=0).T.astype(BF16)


def minus_one_lanes(rows, first):
    lane = lax.broadcasted_iota(jnp.int32, (rows, HEAD_DIM), 1)
    return jnp.where((lane >= first) & (lane < first + 3), -1.0, 0.0).astype(BF16)


def dot_t(a, b):
    return lax.dot_general(a, b, (((1,), (1,)), ((), ())), preferred_element_type=F32)


def dot_n(a, b):
    return lax.dot_general(a, b, (((1,), (0,)), ((), ())), preferred_element_type=F32)


def block_grads(i, j, masked, raw, qr, qt, dot_, ext, dq, dkt, dvt):
    rows = raw.shape[1]
    kb = qr[j, :, 256:384]
    vb = raw[j, :, 384:512]
    ex = ext[i]
    probs, grads = [], []
    for h in range(2):
        ke = jnp.concatenate([kb, minus_one_lanes(rows, 3 * h)], axis=1)
        ve = jnp.concatenate([vb, minus_one_lanes(rows, 6 + 3 * h)], axis=1)
        qe = jnp.concatenate([qr[i, :, h * 128:(h + 1) * 128], ex], axis=1)
        de = jnp.concatenate([raw[i, :, 512 + h * 128:640 + h * 128], ex], axis=1)
        s = dot_t(qe, ke)
        if masked:
            r_id = lax.broadcasted_iota(jnp.int32, s.shape, 0)
            c_id = lax.broadcasted_iota(jnp.int32, s.shape, 1)
            s = jnp.where(r_id >= c_id, s, -jnp.inf)
        p = jnp.exp(s * SM_SCALE)
        ds = (p * dot_t(de, ve)).astype(BF16)
        probs.append(p.astype(BF16))
        grads.append(ds)
        dq[i, :, h * 128:(h + 1) * 128] += dot_n(ds, kb)
    dvt[j] += dot_n(dot_[i], jnp.concatenate(probs, axis=0))
    dkt[j] += dot_n(qt[i], jnp.concatenate(grads, axis=0))


def finish_q(c, raw, qw, tabs, dq, dw):
    cos_t, sin_s = chunk_angles(c, *tabs)
    for h in range(2):
        cols = slice(h * 128, (h + 1) * 128)
        dx, part = norm_rope_grad(raw[c, :, cols].astype(F32), qw[...], cos_t, sin_s, dq[c, :, cols] * SM_SCALE)
        raw[c, :, cols] = dx.astype(BF16)
        dw[0:8, :] += part


def finish_k(c, raw, kw, tabs, dkt, dvt, dw):
    cos_t, sin_s = chunk_angles(c, *tabs)
    dx, part = norm_rope_grad(raw[c, :, 256:384].astype(F32), kw[...], cos_t, sin_s, dkt[c].T * SM_SCALE)
    raw[c, :, 256:384] = dx.astype(BF16)
    dw[8:16, :] += part
    raw[c, :, 384:512] = dvt[c].T.astype(BF16)


def attn_kernel(slab, ld_in, qw, kw, cos_o, sin_o, cos_c, sin_c, out, dw,
                raw, ld, qr, qt, dot_, ext, dq, dkt, dvt, sems):
    n_chunks = raw.shape[0]
    half = n_chunks // 2
    tabs = (cos_o, sin_o, cos_c, sin_c)

    def slot(c):
        dev = jnp.minimum(c, n_chunks - 1 - c)
        return dev, (c >= half).astype(jnp.int32)

    def load(c, start):
        dev, part = slot(c)
        one = pltpu.make_async_copy(slab.at[dev, part], raw.at[c], sems.at[c, 0])
        two = pltpu.make_async_copy(ld_in.at[dev, part], ld.at[c], sems.at[c, 1])
        if start:
            one.start()
            two.start()
        else:
            one.wait()
            two.wait()

    lax.fori_loop(0, n_chunks, lambda c, _: (load(c, True), 0)[1], 0)
    dw[...] = jnp.zeros_like(dw)
    dq[...] = jnp.zeros_like(dq)
    dkt[...] = jnp.zeros_like(dkt)
    dvt[...] = jnp.zeros_like(dvt)

    def prep(c, _):
        load(c, False)
        prep_chunk(c, raw, ld, qw, kw, tabs, qr, qt, dot_, ext)
        return 0

    lax.fori_loop(0, n_chunks, prep, 0)

    def column(j, _):
        block_grads(j, j, True, raw, qr, qt, dot_, ext, dq, dkt, dvt)

        def row(i, _):
            block_grads(i, j, False, raw, qr, qt, dot_, ext, dq, dkt, dvt)
            return 0

        lax.fori_loop(j + 1, n_chunks, row, 0)
        return 0

    lax.fori_loop(0, n_chunks, column, 0)

    def finish(c, _):
        finish_q(c, raw, qw, tabs, dq, dw)
        finish_k(c, raw, kw, tabs, dkt, dvt, dw)
        dev, part = slot(c)
        pltpu.make_async_copy(raw.at[c, :, 0:512], out.at[dev, part], sems.at[c, 0]).start()
        return 0

    lax.fori_loop(0, n_chunks, finish, 0)

    def drain(c, _):
        dev, part = slot(c)
        pltpu.make_async_copy(raw.at[c, :, 0:512], out.at[dev, part], sems.at[c, 0]).wait()
        return 0

    lax.fori_loop(0, n_chunks, drain, 0)


def run_attention(slab, ld, q_norm, k_norm, tabs):
    n_dev, _, rows, _ = slab.shape
    n_chunks = 2 * n_dev
    any_spec = pl.BlockSpec(memory_space=pl.ANY)
    vmem_spec = pl.BlockSpec(memory_space=pltpu.VMEM)
    return pl.pallas_call(
        attn_kernel,
        out_shape=(jax.ShapeDtypeStruct((n_dev, 2, rows, 512), BF16), jax.ShapeDtypeStruct((16, HEAD_DIM), F32)),
        in_specs=[any_spec, any_spec] + [vmem_spec] * 6,
        out_specs=(any_spec, vmem_spec),
        scratch_shapes=[
            pltpu.VMEM((n_chunks, rows, 768), BF16),
            pltpu.VMEM((n_chunks, 8, rows), F32),
            pltpu.VMEM((n_chunks, rows, 384), BF16),
            pltpu.VMEM((n_chunks, HEAD_DIM, 2 * rows), BF16),
            pltpu.VMEM((n_chunks, HEAD_DIM, 2 * rows), BF16),
            pltpu.VMEM((n_chunks, rows, HEAD_DIM), BF16),
            pltpu.VMEM((n_chunks, rows, 256), F32),
            pltpu.VMEM((n_chunks, HEAD_DIM, rows), F32),
            pltpu.VMEM((n_chunks, HEAD_DIM, rows), F32),
            pltpu.SemaphoreType.DMA((n_chunks, 2)),
        ],
        compiler_params=pltpu.CompilerParams(vmem_limit_bytes=67043328),
        name='attention_backward',
    )(slab, ld, q_norm, k_norm, *tabs)


def solution(mesh):
    cp_size = mesh.shape['cp']

    def local_grads(q_raw, k_raw, v_proj, out_fwd, lse_fwd, d_out, q_norm, k_norm):
        local_rows, num_heads = q_raw.shape[0], q_raw.shape[1]
        rows = local_rows // 2
        kv_heads = k_raw.shape[1]
        by_group = lambda a: a.reshape(local_rows, kv_heads, -1)
        slab = jnp.concatenate([by_group(q_raw), by_group(k_raw), by_group(v_proj), by_group(d_out)], axis=-1)
        slab = slab.transpose(1, 0, 2)
        delta = jnp.einsum('thd,thd->th', d_out, out_fwd, preferred_element_type=F32)
        ld = jnp.concatenate([lse_fwd.reshape(local_rows, kv_heads, 2), delta.reshape(local_rows, kv_heads, 2)], axis=-1)
        ld = jnp.pad(ld, ((0, 0), (0, 0), (0, 4))).reshape(2, rows, kv_heads, 8).transpose(2, 0, 3, 1)
        slab = lax.all_to_all(slab, 'cp', 0, 0)
        ld = lax.all_to_all(ld, 'cp', 0, 0)
        slab = slab.reshape(cp_size, 2, rows, 768)
        tabs = angle_tables(jnp.arange(rows)) + angle_tables(jnp.arange(2 * cp_size) * rows)
        out, dw = run_attention(slab, ld, q_norm.reshape(1, -1), k_norm.reshape(1, -1), tabs)
        out = lax.all_to_all(out, 'cp', 0, 0)
        out = out.reshape(kv_heads, local_rows, 512)
        dq_raw = out[..., :256].transpose(1, 0, 2).reshape(local_rows, num_heads, HEAD_DIM)
        dk_raw = out[..., 256:384].transpose(1, 0, 2)
        dv = out[..., 384:].transpose(1, 0, 2)
        dw = lax.psum(jnp.stack([dw[:8].sum(0), dw[8:].sum(0)]), 'cp')
        return dq_raw, dk_raw, dv, dw[0], dw[1]

    row_spec = P(('dp', 'cp'))
    in_specs = (row_spec, row_spec, row_spec, row_spec, row_spec, row_spec, P(), P())
    out_specs = (row_spec, row_spec, row_spec, P('dp'), P('dp'))
    return jax.shard_map(local_grads, mesh=mesh, in_specs=in_specs, out_specs=out_specs, check_vma=False)
```

```python
import functools

import jax
import jax.numpy as jnp
from jax import lax
from jax.experimental import pallas as pl
from jax.experimental.pallas import tpu as pltpu
from jax.sharding import PartitionSpec as P

HEAD_DIM = 128
ROPE_THETA = 1000000.0
NORM_EPS = 1e-6
SM_SCALE = HEAD_DIM ** -0.5
F32 = jnp.float32
BF16 = jnp.bfloat16


def angle_tables(positions):
    inv_freq = ROPE_THETA ** (-jnp.arange(0, HEAD_DIM, 2).astype(F32) / HEAD_DIM)
    angles = positions.astype(F32)[:, None] * inv_freq[None, :]
    angles = jnp.concatenate([angles, angles], axis=-1)
    return jnp.cos(angles), jnp.sin(angles)


def lane_sign():
    lane = lax.broadcasted_iota(jnp.int32, (1, HEAD_DIM), 1)
    return jnp.where(lane < HEAD_DIM // 2, -1.0, 1.0).astype(F32)


def chunk_angles(c, cos_o, sin_o, cos_c, sin_c):
    cc, sc = cos_c[pl.ds(c, 1), :], sin_c[pl.ds(c, 1), :]
    co, so = cos_o[...], sin_o[...]
    return cc * co - sc * so, (sc * co + cc * so) * lane_sign()


def norm_rope(x, weight, cos_t, sin_s):
    rinv = lax.rsqrt(jnp.mean(x * x, axis=-1, keepdims=True) + NORM_EPS)
    y = x * rinv * weight
    return y * cos_t + pltpu.roll(y, HEAD_DIM // 2, 1) * sin_s


def norm_rope_grad(x, weight, cos_t, sin_s, g):
    rinv = lax.rsqrt(jnp.mean(x * x, axis=-1, keepdims=True) + NORM_EPS)
    n = x * rinv
    dy = g * cos_t + pltpu.roll(g * sin_s, HEAD_DIM // 2, 1)
    dw = dy * n
    dn = dy * weight
    dx = rinv * (dn - n * jnp.mean(dn * n, axis=-1, keepdims=True))
    return dx, jnp.sum(dw.reshape(-1, 8, HEAD_DIM), axis=0)


def split3(x):
    hi = x.astype(BF16).astype(F32)
    mid = (x - hi).astype(BF16).astype(F32)
    return hi, mid, x - hi - mid


def prep_chunk(c, src, half, raw, ld, qw, kw, tabs, qr, qt, dot_, ext):
    cos_t, sin_s = chunk_angles(c, *tabs)
    rows = raw.shape[1]
    for h in range(2):
        y = norm_rope(raw[c, :, h * 128:(h + 1) * 128].astype(F32), qw[...], cos_t, sin_s)
        qr[c, :, h * 128:(h + 1) * 128] = y.astype(BF16)
        qt[c, :, h * rows:(h + 1) * rows] = y.T.astype(BF16)
        dot_[c, :, h * rows:(h + 1) * rows] = raw[c, :, 512 + h * 128:640 + h * 128].astype(F32).T.astype(BF16)
    y = norm_rope(raw[c, :, 256:384].astype(F32), kw[...], cos_t, sin_s)
    qr[c, :, 256:384] = y.astype(BF16)
    vals = ld[src, half]
    parts = []
    for t in range(4):
        parts.extend(split3(vals[t:t + 1] * (1.0 / SM_SCALE if t < 2 else 1.0)))
    parts.append(jnp.zeros((HEAD_DIM - 12, rows), F32))
    ext[c] = jnp.concatenate(parts, axis=0).T.astype(BF16)


def minus_one_lanes(rows, first):
    lane = lax.broadcasted_iota(jnp.int32, (rows, HEAD_DIM), 1)
    return jnp.where((lane >= first) & (lane < first + 3), -1.0, 0.0).astype(BF16)


def dot_t(a, b):
    return lax.dot_general(a, b, (((1,), (1,)), ((), ())), preferred_element_type=F32)


def dot_n(a, b):
    return lax.dot_general(a, b, (((1,), (0,)), ((), ())), preferred_element_type=F32)


def block_grads(i, j, masked, raw, qr, qt, dot_, ext, dq, dkt, dvt):
    rows = raw.shape[1]
    kb = qr[j, :, 256:384]
    vb = raw[j, :, 384:512]
    ex = ext[i]
    probs, grads = [], []
    for h in range(2):
        ke = jnp.concatenate([kb, minus_one_lanes(rows, 3 * h)], axis=1)
        ve = jnp.concatenate([vb, minus_one_lanes(rows, 6 + 3 * h)], axis=1)
        qe = jnp.concatenate([qr[i, :, h * 128:(h + 1) * 128], ex], axis=1)
        de = jnp.concatenate([raw[i, :, 512 + h * 128:640 + h * 128], ex], axis=1)
        s = dot_t(qe, ke)
        if masked:
            r_id = lax.broadcasted_iota(jnp.int32, s.shape, 0)
            c_id = lax.broadcasted_iota(jnp.int32, s.shape, 1)
            s = jnp.where(r_id >= c_id, s, -jnp.inf)
        p = jnp.exp(s * SM_SCALE)
        ds = (p * dot_t(de, ve)).astype(BF16)
        probs.append(p.astype(BF16))
        grads.append(ds)
        dq[i, :, h * 128:(h + 1) * 128] += dot_n(ds, kb)
    dvt[j] += dot_n(dot_[i], jnp.concatenate(probs, axis=0))
    dkt[j] += dot_n(qt[i], jnp.concatenate(grads, axis=0))


def finish_q(c, raw, qw, tabs, dq, dw):
    cos_t, sin_s = chunk_angles(c, *tabs)
    for h in range(2):
        cols = slice(h * 128, (h + 1) * 128)
        dx, part = norm_rope_grad(raw[c, :, cols].astype(F32), qw[...], cos_t, sin_s, dq[c, :, cols] * SM_SCALE)
        raw[c, :, cols] = dx.astype(BF16)
        dw[0:8, :] += part


def finish_k(c, raw, kw, tabs, dkt, dvt, dw):
    cos_t, sin_s = chunk_angles(c, *tabs)
    dx, part = norm_rope_grad(raw[c, :, 256:384].astype(F32), kw[...], cos_t, sin_s, dkt[c].T * SM_SCALE)
    raw[c, :, 256:384] = dx.astype(BF16)
    dw[8:16, :] += part
    raw[c, :, 384:512] = dvt[c].T.astype(BF16)


MESH = pl.DeviceIdType.MESH
EARLY = 3


def partner(me, step):
    total = 0
    for bit in (1, 2, 4):
        a, b = (me // bit) % 2, (step // bit) % 2
        total = total + bit * (a + b - 2 * a * b)
    return total


def visit_order(u):
    return u + 2 * ((u // 4) % 2) * (1 - 2 * ((u // 2) % 2))


def attn_kernel(slab, ld_in, qw, kw, cos_o, sin_o, cos_c, sin_c, out, dw_out,
                raw, ld, qr, qt, dot_, ext, dq, dkt, dvt, dw, dw_all,
                send_in, recv_in, send_ld, recv_ld, send_out, recv_out, send_dw, recv_dw, own_sem):
    n_chunks = raw.shape[0]
    n_dev = n_chunks // 2
    me = lax.axis_index('cp')
    tabs = (cos_o, sin_o, cos_c, sin_c)
    block = functools.partial(block_grads, raw=raw, qr=qr, qt=qt, dot_=dot_, ext=ext, dq=dq, dkt=dkt, dvt=dvt)

    def chunk_of(dev, half):
        return dev + half * (n_chunks - 1 - 2 * dev)

    def source(u):
        return partner(me, visit_order(u))

    def in_copy(half, dest, src):
        return pltpu.make_async_remote_copy(
            src_ref=slab.at[dest, half], dst_ref=raw.at[chunk_of(src, half)],
            send_sem=send_in.at[dest, half], recv_sem=recv_in.at[src, half],
            device_id={'cp': dest}, device_id_type=MESH)

    def ld_copy(dest, src):
        return pltpu.make_async_remote_copy(
            src_ref=ld_in.at[dest], dst_ref=ld.at[src],
            send_sem=send_ld.at[dest], recv_sem=recv_ld.at[src],
            device_id={'cp': dest}, device_id_type=MESH)

    def out_parts(part, half, chunk, src):
        cols = (pl.ds(0, 256), pl.ds(256, 256), pl.ds(0, 512))[part]
        return raw.at[chunk, :, cols], out.at[src, half, :, cols]

    def out_copy(part, half, dest, src, chunk):
        a, b = out_parts(part, half, chunk, src)
        return pltpu.make_async_remote_copy(
            src_ref=a, dst_ref=b, send_sem=send_out.at[dest, part], recv_sem=recv_out.at[src, part],
            device_id={'cp': dest}, device_id_type=MESH)

    def own_out(part, half):
        a, b = out_parts(part, half, chunk_of(me, half), me)
        return pltpu.make_async_copy(a, b, own_sem.at[3 + part])

    def dw_copy(dest, src):
        return pltpu.make_async_remote_copy(
            src_ref=dw, dst_ref=dw_all.at[src], send_sem=send_dw.at[dest], recv_sem=recv_dw.at[src],
            device_id={'cp': dest}, device_id_type=MESH)

    def loop(lo, hi, body):
        lax.fori_loop(lo, hi, lambda u, _: (body(u), 0)[1], 0)

    own = [pltpu.make_async_copy(slab.at[me, h], raw.at[chunk_of(me, h)], own_sem.at[h]) for h in range(2)]
    own.append(pltpu.make_async_copy(ld_in.at[me], ld.at[me], own_sem.at[2]))
    for copy in own:
        copy.start()

    barrier = pltpu.get_barrier_semaphore()
    loop(1, n_dev, lambda u: pl.semaphore_signal(barrier, inc=1, device_id={'cp': source(u)}, device_id_type=MESH))
    pl.semaphore_wait(barrier, n_dev - 1)

    loop(1, n_dev, lambda u: ld_copy(source(u), me).start())
    for half in range(2):
        loop(1, n_dev, lambda u, half=half: in_copy(half, source(u), me).start())

    dw[...] = jnp.zeros_like(dw)
    dq[...] = jnp.zeros_like(dq)
    dkt[...] = jnp.zeros_like(dkt)
    dvt[...] = jnp.zeros_like(dvt)
    for copy in own:
        copy.wait()

    def arrive(u, half):
        src = source(u)

        @pl.when(u > 0)
        def _():
            in_copy(half, me, src).wait_recv()
            if half == 0:
                ld_copy(me, src).wait_recv()

        prep_chunk(chunk_of(src, half), src, half, raw, ld, qw, kw, tabs, qr, qt, dot_, ext)

    def send(u, part, half):
        dest = source(u)

        @pl.when(u > 0)
        def _():
            out_copy(part, half, dest, me, chunk_of(dest, half)).start()

        @pl.when(u == 0)
        def _():
            own_out(part, half).start()

    def pair(a, b):
        block(jnp.maximum(a, b), jnp.minimum(a, b), False)

    def diagonal(a):
        block(a, a, True)

    def low_round(u):
        arrive(u, 0)
        a = source(u)
        loop(0, u, lambda w: pair(a, source(w)))
        diagonal(a)

    loop(0, n_dev, low_round)

    def low_queries(u):
        finish_q(source(u), raw, qw, tabs, dq, dw)
        send(u, 0, 0)

    loop(0, n_dev, low_queries)

    def high_round(u):
        arrive(u, 1)
        a = chunk_of(source(u), 1)

        def against(w):
            half = w // n_dev
            pair(a, chunk_of(source(w - half * n_dev), half))

        loop(0, n_dev + u, against)
        diagonal(a)

    loop(0, EARLY, high_round)
    loop(EARLY, n_dev, lambda u: arrive(u, 1))

    def low_column(u):
        j = source(u)
        loop(EARLY, n_dev, lambda w: block(chunk_of(source(w), 1), j, False))
        finish_k(j, raw, kw, tabs, dkt, dvt, dw)
        send(u, 1, 0)

    loop(0, n_dev, low_column)

    def high_finish(u):
        a = chunk_of(source(u), 1)
        loop(jnp.maximum(u + 1, EARLY), n_dev, lambda w: pair(a, chunk_of(source(w), 1)))

        @pl.when(u >= EARLY)
        def _():
            diagonal(a)

        finish_q(a, raw, qw, tabs, dq, dw)
        finish_k(a, raw, kw, tabs, dkt, dvt, dw)
        send(u, 2, 1)

    loop(0, n_dev, high_finish)

    loop(1, n_dev, lambda u: dw_copy(source(u), me).start())
    dw_all[me] = dw[...]

    def settle(u):
        src = source(u)
        ld_copy(src, me).wait_send()
        for half in range(2):
            in_copy(half, src, me).wait_send()
        for part in range(3):
            out_copy(part, part // 2, src, me, chunk_of(src, part // 2)).wait_send()
            out_copy(part, part // 2, me, src, chunk_of(me, part // 2)).wait_recv()
        dw_copy(src, me).wait_send()
        dw_copy(me, src).wait_recv()

    loop(1, n_dev, settle)
    for part in range(3):
        own_out(part, part // 2).wait()
    total = dw_all[0]
    for src in range(1, n_dev):
        total = total + dw_all[src]
    dw_out[...] = total


def run_attention(slab, ld, q_norm, k_norm, tabs):
    n_dev, _, rows, _ = slab.shape
    n_chunks = 2 * n_dev
    any_spec = pl.BlockSpec(memory_space=pl.ANY)
    vmem_spec = pl.BlockSpec(memory_space=pltpu.VMEM)
    dma = pltpu.SemaphoreType.DMA
    return pl.pallas_call(
        attn_kernel,
        out_shape=(jax.ShapeDtypeStruct((n_dev, 2, rows, 512), BF16), jax.ShapeDtypeStruct((16, HEAD_DIM), F32)),
        in_specs=[any_spec, any_spec] + [vmem_spec] * 6,
        out_specs=(any_spec, vmem_spec),
        scratch_shapes=[
            pltpu.VMEM((n_chunks, rows, 768), BF16),
            pltpu.VMEM((n_dev, 2, 8, rows), F32),
            pltpu.VMEM((n_chunks, rows, 384), BF16),
            pltpu.VMEM((n_chunks, HEAD_DIM, 2 * rows), BF16),
            pltpu.VMEM((n_chunks, HEAD_DIM, 2 * rows), BF16),
            pltpu.VMEM((n_chunks, rows, HEAD_DIM), BF16),
            pltpu.VMEM((n_chunks, rows, 256), F32),
            pltpu.VMEM((n_chunks, HEAD_DIM, rows), F32),
            pltpu.VMEM((n_chunks, HEAD_DIM, rows), F32),
            pltpu.VMEM((16, HEAD_DIM), F32),
            pltpu.VMEM((n_dev, 16, HEAD_DIM), F32),
            dma((n_dev, 2)), dma((n_dev, 2)), dma((n_dev,)), dma((n_dev,)),
            dma((n_dev, 3)), dma((n_dev, 3)), dma((n_dev,)), dma((n_dev,)), dma((6,)),
        ],
        compiler_params=pltpu.CompilerParams(vmem_limit_bytes=67043328, collective_id=0, has_side_effects=True),
        name='attention_backward',
    )(slab, ld, q_norm, k_norm, *tabs)


def pack_kernel(q, k, v, o, lse, do, slab, ld, wide):
    rows, heads = q.shape[0], q.shape[1]
    groups = k.shape[1]

    def scatter(x, n_heads, col):
        per = n_heads // groups
        wide[0:rows * n_heads, :] = x[...].reshape(rows * n_heads, HEAD_DIM).astype(F32)
        for h in range(n_heads):
            first = col + (h % per) * HEAD_DIM
            slab[h // per, :, first:first + HEAD_DIM] = wide[pl.ds(h, rows, stride=n_heads), :].astype(BF16)

    scatter(q, heads, 0)
    scatter(k, groups, 256)
    scatter(v, groups, 384)
    scatter(do, heads, 512)
    lse_t = lse[...].T
    delta_t = jnp.sum(do[...].astype(F32) * o[...].astype(F32), axis=-1).T
    for g in range(groups):
        ld[g, 0] = jnp.concatenate([lse_t[2 * g:2 * g + 2], delta_t[2 * g:2 * g + 2], jnp.zeros((4, rows), F32)], axis=0)


def pack_inputs(q, k, v, o, lse, do):
    local_rows, heads, _ = q.shape
    groups = k.shape[1]
    blk = min(128, local_rows // 2)
    per_half = local_rows // 2 // blk
    big = pl.BlockSpec((blk, heads, HEAD_DIM), lambda i: (i, 0, 0))
    small = pl.BlockSpec((blk, groups, HEAD_DIM), lambda i: (i, 0, 0))
    return pl.pallas_call(
        pack_kernel,
        grid=(local_rows // blk,),
        in_specs=[big, small, small, big, pl.BlockSpec((blk, heads), lambda i: (i, 0)), big],
        out_specs=(pl.BlockSpec((groups, blk, 768), lambda i: (0, i, 0)),
                   pl.BlockSpec((groups, 1, 8, blk), lambda i: (0, i // per_half, 0, i % per_half))),
        out_shape=(jax.ShapeDtypeStruct((groups, local_rows, 768), BF16),
                   jax.ShapeDtypeStruct((groups, 2, 8, local_rows // 2), F32)),
        scratch_shapes=[pltpu.VMEM((blk * heads, HEAD_DIM), F32)],
        name='pack_inputs',
    )(q, k, v, o, lse, do)


def unpack_kernel(out, dq, dk, dv, wide):
    rows, heads = dq.shape[0], dq.shape[1]
    groups = dk.shape[1]

    def gather(dst, n_heads, col):
        per = n_heads // groups
        for h in range(n_heads):
            first = col + (h % per) * HEAD_DIM
            wide[pl.ds(h, rows, stride=n_heads), :] = out[h // per, :, first:first + HEAD_DIM].astype(F32)
        dst[...] = wide[0:rows * n_heads, :].astype(BF16).reshape(rows, n_heads, HEAD_DIM)

    gather(dq, heads, 0)
    gather(dk, groups, 256)
    gather(dv, groups, 384)


def unpack_outputs(out, heads):
    groups, local_rows, _ = out.shape
    blk = min(128, local_rows // 2)
    big = pl.BlockSpec((blk, heads, HEAD_DIM), lambda i: (i, 0, 0))
    small = pl.BlockSpec((blk, groups, HEAD_DIM), lambda i: (i, 0, 0))
    return pl.pallas_call(
        unpack_kernel,
        grid=(local_rows // blk,),
        in_specs=[pl.BlockSpec((groups, blk, 512), lambda i: (0, i, 0))],
        out_specs=(big, small, small),
        out_shape=(jax.ShapeDtypeStruct((local_rows, heads, HEAD_DIM), BF16),
                   jax.ShapeDtypeStruct((local_rows, groups, HEAD_DIM), BF16),
                   jax.ShapeDtypeStruct((local_rows, groups, HEAD_DIM), BF16)),
        scratch_shapes=[pltpu.VMEM((blk * heads, HEAD_DIM), F32)],
        name='unpack_outputs',
    )(out)


def solution(mesh):
    cp_size = mesh.shape['cp']

    def local_grads(q_raw, k_raw, v_proj, out_fwd, lse_fwd, d_out, q_norm, k_norm):
        local_rows, num_heads = q_raw.shape[0], q_raw.shape[1]
        rows = local_rows // 2
        tabs = angle_tables(jnp.arange(rows)) + angle_tables(jnp.arange(2 * cp_size) * rows)
        slab, ld = pack_inputs(q_raw, k_raw, v_proj, out_fwd, lse_fwd, d_out)
        out, dw = run_attention(slab.reshape(cp_size, 2, rows, 768), ld, q_norm.reshape(1, -1), k_norm.reshape(1, -1), tabs)
        dq_raw, dk_raw, dv = unpack_outputs(out.reshape(cp_size, local_rows, 512), num_heads)
        return dq_raw, dk_raw, dv, dw[:8].sum(0), dw[8:].sum(0)

    row_spec = P(('dp', 'cp'))
    in_specs = (row_spec, row_spec, row_spec, row_spec, row_spec, row_spec, P(), P())
    out_specs = (row_spec, row_spec, row_spec, P('dp'), P('dp'))
    return jax.shard_map(local_grads, mesh=mesh, in_specs=in_specs, out_specs=out_specs, check_vma=False)
```

```python
import functools

import jax
import jax.numpy as jnp
from jax import lax
from jax.experimental import pallas as pl
from jax.experimental.pallas import tpu as pltpu
from jax.sharding import PartitionSpec as P

HEAD_DIM = 128
ROPE_THETA = 1000000.0
NORM_EPS = 1e-6
SM_SCALE = HEAD_DIM ** -0.5
F32 = jnp.float32
BF16 = jnp.bfloat16


def angle_tables(positions):
    inv_freq = ROPE_THETA ** (-jnp.arange(0, HEAD_DIM, 2).astype(F32) / HEAD_DIM)
    angles = positions.astype(F32)[:, None] * inv_freq[None, :]
    angles = jnp.concatenate([angles, angles], axis=-1)
    return jnp.cos(angles), jnp.sin(angles)


def lane_sign():
    lane = lax.broadcasted_iota(jnp.int32, (1, HEAD_DIM), 1)
    return jnp.where(lane < HEAD_DIM // 2, -1.0, 1.0).astype(F32)


def chunk_angles(c, cos_o, sin_o, cos_c, sin_c):
    cc, sc = cos_c[pl.ds(c, 1), :], sin_c[pl.ds(c, 1), :]
    co, so = cos_o[...], sin_o[...]
    return cc * co - sc * so, (sc * co + cc * so) * lane_sign()


def norm_rope(x, weight, cos_t, sin_s):
    rinv = lax.rsqrt(jnp.mean(x * x, axis=-1, keepdims=True) + NORM_EPS)
    y = x * rinv * weight
    return y * cos_t + pltpu.roll(y, HEAD_DIM // 2, 1) * sin_s


def norm_rope_grad(x, weight, cos_t, sin_s, g):
    rinv = lax.rsqrt(jnp.mean(x * x, axis=-1, keepdims=True) + NORM_EPS)
    n = x * rinv
    dy = g * cos_t + pltpu.roll(g * sin_s, HEAD_DIM // 2, 1)
    dw = dy * n
    dn = dy * weight
    dx = rinv * (dn - n * jnp.mean(dn * n, axis=-1, keepdims=True))
    return dx, jnp.sum(dw.reshape(-1, 8, HEAD_DIM), axis=0)


def split3(x):
    hi = x.astype(BF16).astype(F32)
    mid = (x - hi).astype(BF16).astype(F32)
    return hi, mid, x - hi - mid


def prep_chunk(c, src, half, raw, ld, qw, kw, tabs, qr, qt, dot_, kt, ext):
    cos_t, sin_s = chunk_angles(c, *tabs)
    rows = raw.shape[1]
    for h in range(2):
        y = norm_rope(raw[c, :, h * 128:(h + 1) * 128].astype(F32), qw[...], cos_t, sin_s)
        qr[c, :, h * 128:(h + 1) * 128] = y.astype(BF16)
        qt[c, :, h * rows:(h + 1) * rows] = y.astype(BF16).T
        dot_[c, :, h * rows:(h + 1) * rows] = raw[c, :, 512 + h * 128:640 + h * 128].T
    y = norm_rope(raw[c, :, 256:384].astype(F32), kw[...], cos_t, sin_s)
    qr[c, :, 256:384] = y.astype(BF16)
    kt[c] = y.astype(BF16).T
    vals = ld[src, half]
    for h in range(2):
        parts = list(split3(vals[h:h + 1] * (1.0 / SM_SCALE))) + list(split3(vals[2 + h:3 + h]))
        parts.append(jnp.zeros((HEAD_DIM - 6, rows), F32))
        ext[c, :, h * 128:(h + 1) * 128] = jnp.concatenate(parts, axis=0).astype(BF16).T


def minus_one_lanes(rows, first):
    lane = lax.broadcasted_iota(jnp.int32, (rows, HEAD_DIM), 1)
    return jnp.where((lane >= first) & (lane < first + 3), -1.0, 0.0).astype(BF16)


def dot_t(a, b):
    return lax.dot_general(a, b, (((1,), (1,)), ((), ())), preferred_element_type=F32)


def dot_n(a, b):
    return lax.dot_general(a, b, (((1,), (0,)), ((), ())), preferred_element_type=F32)


def tile_grads(i, j, q0, qn, kn, masked, raw, qr, qt, dot_, kt, ext, dqt, dkt, dvt):
    rows = raw.shape[1]
    ke = jnp.concatenate([qr[j, 0:kn, 256:384], minus_one_lanes(kn, 0)], axis=1)
    ve = jnp.concatenate([raw[j, 0:kn, 384:512], minus_one_lanes(kn, 3)], axis=1)
    span = slice(q0, q0 + qn)
    ex = jnp.concatenate([ext[i, span, 0:128], ext[i, span, 128:256]], axis=0)
    q_all = jnp.concatenate([qr[i, span, 0:128], qr[i, span, 128:256]], axis=0)
    do_all = jnp.concatenate([raw[i, span, 512:640], raw[i, span, 640:768]], axis=0)
    s = dot_t(jnp.concatenate([q_all, ex], axis=1), ke)
    if masked:
        r_id = lax.rem(lax.broadcasted_iota(jnp.int32, s.shape, 0), qn) + q0
        c_id = lax.broadcasted_iota(jnp.int32, s.shape, 1)
        s = jnp.where(r_id >= c_id, s, -jnp.inf)
    p = jnp.exp(s * SM_SCALE)
    ds = (p * dot_t(jnp.concatenate([do_all, ex], axis=1), ve)).astype(BF16)
    spans = [slice(h * rows + q0, h * rows + q0 + qn) for h in range(2)]
    both = lambda ref: jnp.concatenate([ref[i, :, cols] for cols in spans], axis=1)
    dvt[j, :, 0:kn] += dot_n(both(dot_), p.astype(BF16))
    dkt[j, :, 0:kn] += dot_n(both(qt), ds)
    dq_part = dot_t(kt[j, :, 0:kn], ds)
    for h in range(2):
        dqt[i, :, spans[h]] += dq_part[:, h * qn:(h + 1) * qn]


def block_grads(i, j, **refs):
    rows = refs['raw'].shape[1]
    for q0 in (0, rows // 2):
        tile_grads(i, j, q0, rows // 2, rows, False, **refs)


def diagonal_grads(i, **refs):
    half = refs['raw'].shape[1] // 2
    tile_grads(i, i, 0, half, half, True, **refs)
    tile_grads(i, i, half, half, 2 * half, True, **refs)


def finish_q(c, raw, qw, tabs, dqt, dw):
    cos_t, sin_s = chunk_angles(c, *tabs)
    rows = raw.shape[1]
    for h in range(2):
        cols = slice(h * 128, (h + 1) * 128)
        grad = dqt[c, :, h * rows:(h + 1) * rows].T * SM_SCALE
        dx, part = norm_rope_grad(raw[c, :, cols].astype(F32), qw[...], cos_t, sin_s, grad)
        raw[c, :, cols] = dx.astype(BF16)
        dw[0:8, :] += part


def finish_k(c, raw, kw, tabs, dkt, dvt, dw):
    cos_t, sin_s = chunk_angles(c, *tabs)
    dx, part = norm_rope_grad(raw[c, :, 256:384].astype(F32), kw[...], cos_t, sin_s, dkt[c].T * SM_SCALE)
    raw[c, :, 256:384] = dx.astype(BF16)
    dw[8:16, :] += part
    raw[c, :, 384:512] = dvt[c].T.astype(BF16)


MESH = pl.DeviceIdType.MESH
EARLY = 5


def partner(me, step):
    total = me + step
    for bit in (1, 2, 4):
        total = total - 2 * bit * lax.rem(lax.div(me, bit), 2) * lax.rem(lax.div(step, bit), 2)
    return total


def visit_order(u):
    return u + 2 * lax.div(u, 4) * (1 - 2 * lax.rem(lax.div(u, 2), 2))


def attn_kernel(slab, ld_in, qw, kw, cos_o, sin_o, cos_c, sin_c, out, dw_out,
                raw, ld, qr, qt, dot_, kt, ext, dqt, dkt, dvt, dw, dw_all,
                send_in, recv_in, send_ld, recv_ld, send_out, recv_out, send_dw, recv_dw, own_sem):
    n_chunks = raw.shape[0]
    n_dev = n_chunks // 2
    me = lax.axis_index('cp')
    tabs = (cos_o, sin_o, cos_c, sin_c)
    refs = dict(raw=raw, qr=qr, qt=qt, dot_=dot_, kt=kt, ext=ext, dqt=dqt, dkt=dkt, dvt=dvt)
    block = functools.partial(block_grads, **refs)
    diagonal = functools.partial(diagonal_grads, **refs)

    def chunk_of(dev, half):
        return dev + half * (n_chunks - 1 - 2 * dev)

    def source(u):
        return partner(me, visit_order(jnp.int32(u)))

    def in_copy(half, dest, src):
        return pltpu.make_async_remote_copy(
            src_ref=slab.at[dest, half], dst_ref=raw.at[chunk_of(src, half)],
            send_sem=send_in.at[dest, half], recv_sem=recv_in.at[src, half],
            device_id={'cp': dest}, device_id_type=MESH)

    def ld_copy(dest, src):
        return pltpu.make_async_remote_copy(
            src_ref=ld_in.at[dest], dst_ref=ld.at[src],
            send_sem=send_ld.at[dest], recv_sem=recv_ld.at[src],
            device_id={'cp': dest}, device_id_type=MESH)

    def out_parts(part, half, chunk, src):
        cols = (pl.ds(0, 256), pl.ds(256, 256), pl.ds(0, 512))[part]
        return raw.at[chunk, :, cols], out.at[src, half, :, cols]

    def out_copy(part, half, dest, src, chunk):
        a, b = out_parts(part, half, chunk, src)
        return pltpu.make_async_remote_copy(
            src_ref=a, dst_ref=b, send_sem=send_out.at[dest, part], recv_sem=recv_out.at[src, part],
            device_id={'cp': dest}, device_id_type=MESH)

    def own_out(part, half):
        a, b = out_parts(part, half, chunk_of(me, half), me)
        return pltpu.make_async_copy(a, b, own_sem.at[3 + part])

    def dw_copy(dest, src):
        return pltpu.make_async_remote_copy(
            src_ref=dw, dst_ref=dw_all.at[src], send_sem=send_dw.at[dest], recv_sem=recv_dw.at[src],
            device_id={'cp': dest}, device_id_type=MESH)

    def loop(lo, hi, body):
        lax.fori_loop(lo, hi, lambda u, _: (body(u), 0)[1], 0)

    def loop_by_two(lo, hi, body):
        count = hi - lo

        def two(m):
            body(lo + 2 * m)
            body(lo + 2 * m + 1)

        loop(0, count // 2, two)

        @pl.when(count % 2 == 1)
        def _():
            body(hi - 1)

    own = [pltpu.make_async_copy(slab.at[me, h], raw.at[chunk_of(me, h)], own_sem.at[h]) for h in range(2)]
    own.append(pltpu.make_async_copy(ld_in.at[me], ld.at[me], own_sem.at[2]))
    for copy in own:
        copy.start()

    barrier = pltpu.get_barrier_semaphore()
    loop(1, n_dev, lambda u: pl.semaphore_signal(barrier, inc=1, device_id={'cp': source(u)}, device_id_type=MESH))
    pl.semaphore_wait(barrier, n_dev - 1)

    loop(1, n_dev, lambda u: ld_copy(source(u), me).start())
    for half in range(2):
        in_copy(half, source(1), me).start()
    for half in range(2):
        loop(2, n_dev, lambda u, half=half: in_copy(half, source(u), me).start())

    dw[...] = jnp.zeros_like(dw)
    dqt[...] = jnp.zeros_like(dqt)
    dkt[...] = jnp.zeros_like(dkt)
    dvt[...] = jnp.zeros_like(dvt)
    for copy in own:
        copy.wait()

    def arrive(t):
        visit, half = stop(t)
        src = source(visit)

        @pl.when(visit > 0)
        def _():
            in_copy(half, me, src).wait_recv()

        @pl.when((visit > 0) & (half == 0))
        def _():
            ld_copy(me, src).wait_recv()

        prep_chunk(chunk_of(src, half), src, half, raw, ld, qw, kw, tabs, qr, qt, dot_, kt, ext)

    def send(u, part, half):
        dest = source(u)

        @pl.when(u > 0)
        def _():
            out_copy(part, half, dest, me, chunk_of(dest, half)).start()

        @pl.when(u == 0)
        def _():
            own_out(part, half).start()

    def stop(t):
        t = jnp.int32(t)
        late = lax.div(t + 12, 16)
        visit = (1 - late) * lax.rem(t, 2) + late * (2 + lax.rem(t + 2, 6))
        half = (1 - late) * lax.div(t, 2) + late * (lax.div(t + 2, 6) - 1)
        return visit, half

    def chunk_at(t):
        visit, half = stop(t)
        return chunk_of(source(visit), half)

    def pair(a, b):
        block(jnp.maximum(a, b), jnp.minimum(a, b))

    def row_round(t):
        arrive(t)
        a = chunk_at(t)
        loop_by_two(0, t, lambda w: pair(a, chunk_at(w)))
        diagonal(a)

    n_low = n_dev + 2
    n_row = n_low + EARLY - 2
    loop(0, n_low, row_round)

    def low_queries(u):
        finish_q(source(u), raw, qw, tabs, dqt, dw)
        send(u, 0, 0)

    loop(0, n_dev, low_queries)
    loop(n_low, n_row, row_round)
    loop(n_row, n_chunks, arrive)

    def low_column(u):
        j = source(u)
        for w in range(n_row, n_chunks):
            block(chunk_at(w), j)
        finish_k(j, raw, kw, tabs, dkt, dvt, dw)
        send(u, 1, 0)

    loop(0, n_dev, low_column)

    def high_finish(u):
        a = chunk_of(source(u), 1)
        loop_by_two(jnp.maximum(u + 1, EARLY), n_dev, lambda w: pair(a, chunk_of(source(w), 1)))

        @pl.when(u >= EARLY)
        def _():
            diagonal(a)

        finish_q(a, raw, qw, tabs, dqt, dw)
        finish_k(a, raw, kw, tabs, dkt, dvt, dw)
        send(u, 2, 1)

    loop(0, n_dev, high_finish)

    loop(1, n_dev, lambda u: dw_copy(source(u), me).start())
    dw_all[me] = dw[...]

    def settle(u):
        src = source(u)
        ld_copy(src, me).wait_send()
        for half in range(2):
            in_copy(half, src, me).wait_send()
        for part in range(3):
            out_copy(part, part // 2, src, me, chunk_of(src, part // 2)).wait_send()
            out_copy(part, part // 2, me, src, chunk_of(me, part // 2)).wait_recv()
        dw_copy(src, me).wait_send()
        dw_copy(me, src).wait_recv()

    loop(1, n_dev, settle)
    for part in range(3):
        own_out(part, part // 2).wait()
    total = dw_all[0]
    for src in range(1, n_dev):
        total = total + dw_all[src]
    dw_out[...] = total


def run_attention(slab, ld, q_norm, k_norm, tabs):
    n_dev, _, rows, _ = slab.shape
    n_chunks = 2 * n_dev
    any_spec = pl.BlockSpec(memory_space=pl.ANY)
    vmem_spec = pl.BlockSpec(memory_space=pltpu.VMEM)
    dma = pltpu.SemaphoreType.DMA
    return pl.pallas_call(
        attn_kernel,
        out_shape=(jax.ShapeDtypeStruct((n_dev, 2, rows, 512), BF16), jax.ShapeDtypeStruct((16, HEAD_DIM), F32)),
        in_specs=[any_spec, any_spec] + [vmem_spec] * 6,
        out_specs=(any_spec, vmem_spec),
        scratch_shapes=[
            pltpu.VMEM((n_chunks, rows, 768), BF16),
            pltpu.VMEM((n_dev, 2, 8, rows), F32),
            pltpu.VMEM((n_chunks, rows, 384), BF16),
            pltpu.VMEM((n_chunks, HEAD_DIM, 2 * rows), BF16),
            pltpu.VMEM((n_chunks, HEAD_DIM, 2 * rows), BF16),
            pltpu.VMEM((n_chunks, HEAD_DIM, rows), BF16),
            pltpu.VMEM((n_chunks, rows, 256), BF16),
            pltpu.VMEM((n_chunks, HEAD_DIM, 2 * rows), F32),
            pltpu.VMEM((n_chunks, HEAD_DIM, rows), F32),
            pltpu.VMEM((n_chunks, HEAD_DIM, rows), F32),
            pltpu.VMEM((16, HEAD_DIM), F32),
            pltpu.VMEM((n_dev, 16, HEAD_DIM), F32),
            dma((n_dev, 2)), dma((n_dev, 2)), dma((n_dev,)), dma((n_dev,)),
            dma((n_dev, 3)), dma((n_dev, 3)), dma((n_dev,)), dma((n_dev,)), dma((6,)),
        ],
        compiler_params=pltpu.CompilerParams(vmem_limit_bytes=67043328, collective_id=0, has_side_effects=True),
        name='attention_backward',
    )(slab, ld, q_norm, k_norm, *tabs)


def pack_kernel(q, k, v, o, lse, do, slab, ld, wide):
    rows, heads = q.shape[0], q.shape[1]
    groups = k.shape[1]

    def scatter(x, n_heads, col):
        per = n_heads // groups
        wide[0:rows * n_heads, :] = x[...].reshape(rows * n_heads, HEAD_DIM).astype(F32)
        for h in range(n_heads):
            first = col + (h % per) * HEAD_DIM
            slab[h // per, :, first:first + HEAD_DIM] = wide[pl.ds(h, rows, stride=n_heads), :].astype(BF16)

    scatter(q, heads, 0)
    scatter(k, groups, 256)
    scatter(v, groups, 384)
    scatter(do, heads, 512)
    lse_t = lse[...].T
    delta_t = jnp.sum(do[...].astype(F32) * o[...].astype(F32), axis=-1).T
    for g in range(groups):
        ld[g, 0] = jnp.concatenate([lse_t[2 * g:2 * g + 2], delta_t[2 * g:2 * g + 2], jnp.zeros((4, rows), F32)], axis=0)


def pack_inputs(q, k, v, o, lse, do):
    local_rows, heads, _ = q.shape
    groups = k.shape[1]
    blk = min(128, local_rows // 2)
    per_half = local_rows // 2 // blk
    big = pl.BlockSpec((blk, heads, HEAD_DIM), lambda i: (i, 0, 0))
    small = pl.BlockSpec((blk, groups, HEAD_DIM), lambda i: (i, 0, 0))
    return pl.pallas_call(
        pack_kernel,
        grid=(local_rows // blk,),
        in_specs=[big, small, small, big, pl.BlockSpec((blk, heads), lambda i: (i, 0)), big],
        out_specs=(pl.BlockSpec((groups, blk, 768), lambda i: (0, i, 0)),
                   pl.BlockSpec((groups, 1, 8, blk), lambda i: (0, i // per_half, 0, i % per_half))),
        out_shape=(jax.ShapeDtypeStruct((groups, local_rows, 768), BF16),
                   jax.ShapeDtypeStruct((groups, 2, 8, local_rows // 2), F32)),
        scratch_shapes=[pltpu.VMEM((blk * heads, HEAD_DIM), F32)],
        name='pack_inputs',
    )(q, k, v, o, lse, do)


def unpack_kernel(out, dq, dk, dv, wide):
    rows, heads = dq.shape[0], dq.shape[1]
    groups = dk.shape[1]

    def gather(dst, n_heads, col):
        per = n_heads // groups
        for h in range(n_heads):
            first = col + (h % per) * HEAD_DIM
            wide[pl.ds(h, rows, stride=n_heads), :] = out[h // per, :, first:first + HEAD_DIM].astype(F32)
        dst[...] = wide[0:rows * n_heads, :].astype(BF16).reshape(rows, n_heads, HEAD_DIM)

    gather(dq, heads, 0)
    gather(dk, groups, 256)
    gather(dv, groups, 384)


def unpack_outputs(out, heads):
    groups, local_rows, _ = out.shape
    blk = min(128, local_rows // 2)
    big = pl.BlockSpec((blk, heads, HEAD_DIM), lambda i: (i, 0, 0))
    small = pl.BlockSpec((blk, groups, HEAD_DIM), lambda i: (i, 0, 0))
    return pl.pallas_call(
        unpack_kernel,
        grid=(local_rows // blk,),
        in_specs=[pl.BlockSpec((groups, blk, 512), lambda i: (0, i, 0))],
        out_specs=(big, small, small),
        out_shape=(jax.ShapeDtypeStruct((local_rows, heads, HEAD_DIM), BF16),
                   jax.ShapeDtypeStruct((local_rows, groups, HEAD_DIM), BF16),
                   jax.ShapeDtypeStruct((local_rows, groups, HEAD_DIM), BF16)),
        scratch_shapes=[pltpu.VMEM((blk * heads, HEAD_DIM), F32)],
        name='unpack_outputs',
    )(out)


def solution(mesh):
    cp_size = mesh.shape['cp']

    def local_grads(q_raw, k_raw, v_proj, out_fwd, lse_fwd, d_out, q_norm, k_norm):
        local_rows, num_heads = q_raw.shape[0], q_raw.shape[1]
        rows = local_rows // 2
        tabs = angle_tables(jnp.arange(rows)) + angle_tables(jnp.arange(2 * cp_size) * rows)
        slab, ld = pack_inputs(q_raw, k_raw, v_proj, out_fwd, lse_fwd, d_out)
        out, dw = run_attention(slab.reshape(cp_size, 2, rows, 768), ld, q_norm.reshape(1, -1), k_norm.reshape(1, -1), tabs)
        dq_raw, dk_raw, dv = unpack_outputs(out.reshape(cp_size, local_rows, 512), num_heads)
        return dq_raw, dk_raw, dv, dw[:8].sum(0), dw[8:].sum(0)

    row_spec = P(('dp', 'cp'))
    in_specs = (row_spec, row_spec, row_spec, row_spec, row_spec, row_spec, P(), P())
    out_specs = (row_spec, row_spec, row_spec, P('dp'), P('dp'))
    return jax.shard_map(local_grads, mesh=mesh, in_specs=in_specs, out_specs=out_specs, check_vma=False)
```

```python
import functools

import jax
import jax.numpy as jnp
from jax import lax
from jax.experimental import pallas as pl
from jax.experimental.pallas import tpu as pltpu
from jax.sharding import PartitionSpec as P

HEAD_DIM = 128
ROPE_THETA = 1000000.0
NORM_EPS = 1e-6
SM_SCALE = HEAD_DIM ** -0.5
F32 = jnp.float32
BF16 = jnp.bfloat16


def angle_tables(positions):
    inv_freq = ROPE_THETA ** (-jnp.arange(0, HEAD_DIM, 2).astype(F32) / HEAD_DIM)
    angles = positions.astype(F32)[:, None] * inv_freq[None, :]
    angles = jnp.concatenate([angles, angles], axis=-1)
    return jnp.cos(angles), jnp.sin(angles)


def lane_sign():
    lane = lax.broadcasted_iota(jnp.int32, (1, HEAD_DIM), 1)
    return jnp.where(lane < HEAD_DIM // 2, -1.0, 1.0).astype(F32)


def chunk_angles(c, cos_o, sin_o, cos_c, sin_c):
    cc, sc = cos_c[pl.ds(c, 1), :], sin_c[pl.ds(c, 1), :]
    co, so = cos_o[...], sin_o[...]
    return cc * co - sc * so, (sc * co + cc * so) * lane_sign()


def norm_rope(x, weight, cos_t, sin_s):
    rinv = lax.rsqrt(jnp.mean(x * x, axis=-1, keepdims=True) + NORM_EPS)
    y = x * rinv * weight
    return y * cos_t + pltpu.roll(y, HEAD_DIM // 2, 1) * sin_s


def norm_rope_grad(x, weight, cos_t, sin_s, g):
    rinv = lax.rsqrt(jnp.mean(x * x, axis=-1, keepdims=True) + NORM_EPS)
    n = x * rinv
    dy = g * cos_t + pltpu.roll(g * sin_s, HEAD_DIM // 2, 1)
    dw = dy * n
    dn = dy * weight
    dx = rinv * (dn - n * jnp.mean(dn * n, axis=-1, keepdims=True))
    return dx, jnp.sum(dw.reshape(-1, 8, HEAD_DIM), axis=0)


def split3(x):
    hi = x.astype(BF16).astype(F32)
    mid = (x - hi).astype(BF16).astype(F32)
    return hi, mid, x - hi - mid


def prep_chunk(c, src, half, raw, ld, qw, kw, tabs, qr, qt, dot_, kt, ext):
    cos_t, sin_s = chunk_angles(c, *tabs)
    rows = raw.shape[1]
    for h in range(2):
        y = norm_rope(raw[c, :, h * 128:(h + 1) * 128].astype(F32), qw[...], cos_t, sin_s)
        qr[c, :, h * 128:(h + 1) * 128] = y.astype(BF16)
        qt[c, :, h * rows:(h + 1) * rows] = y.astype(BF16).T
        dot_[c, :, h * rows:(h + 1) * rows] = raw[c, :, 512 + h * 128:640 + h * 128].T
    y = norm_rope(raw[c, :, 256:384].astype(F32), kw[...], cos_t, sin_s)
    qr[c, :, 256:384] = y.astype(BF16)
    kt[c] = y.astype(BF16).T
    vals = ld[src, half]
    for h in range(2):
        parts = list(split3(vals[h:h + 1] * (1.0 / SM_SCALE))) + list(split3(vals[2 + h:3 + h]))
        parts.append(jnp.zeros((HEAD_DIM - 6, rows), F32))
        ext[c, :, h * 128:(h + 1) * 128] = jnp.concatenate(parts, axis=0).astype(BF16).T


def minus_one_lanes(rows, first):
    lane = lax.broadcasted_iota(jnp.int32, (rows, HEAD_DIM), 1)
    return jnp.where((lane >= first) & (lane < first + 3), -1.0, 0.0).astype(BF16)


def dot_t(a, b):
    return lax.dot_general(a, b, (((1,), (1,)), ((), ())), preferred_element_type=F32)


def dot_n(a, b):
    return lax.dot_general(a, b, (((1,), (0,)), ((), ())), preferred_element_type=F32)


def tile_grads(i, j, q0, qn, kn, masked, raw, qr, qt, dot_, kt, ext, dqt, dkt, dvt):
    rows = raw.shape[1]
    ke = jnp.concatenate([qr[j, 0:kn, 256:384], minus_one_lanes(kn, 0)], axis=1)
    ve = jnp.concatenate([raw[j, 0:kn, 384:512], minus_one_lanes(kn, 3)], axis=1)
    span = slice(q0, q0 + qn)
    ex = jnp.concatenate([ext[i, span, 0:128], ext[i, span, 128:256]], axis=0)
    q_all = jnp.concatenate([qr[i, span, 0:128], qr[i, span, 128:256]], axis=0)
    do_all = jnp.concatenate([raw[i, span, 512:640], raw[i, span, 640:768]], axis=0)
    s = dot_t(jnp.concatenate([q_all, ex], axis=1), ke)
    if masked:
        r_id = lax.rem(lax.broadcasted_iota(jnp.int32, s.shape, 0), qn) + q0
        c_id = lax.broadcasted_iota(jnp.int32, s.shape, 1)
        s = jnp.where(r_id >= c_id, s, -jnp.inf)
    p = jnp.exp(s * SM_SCALE)
    ds = (p * dot_t(jnp.concatenate([do_all, ex], axis=1), ve)).astype(BF16)
    spans = [slice(h * rows + q0, h * rows + q0 + qn) for h in range(2)]
    both = lambda ref: jnp.concatenate([ref[i, :, cols] for cols in spans], axis=1)
    dvt[j, :, 0:kn] += dot_n(both(dot_), p.astype(BF16))
    dkt[j, :, 0:kn] += dot_n(both(qt), ds)
    dq_part = dot_t(kt[j, :, 0:kn], ds)
    for h in range(2):
        dqt[i, :, spans[h]] += dq_part[:, h * qn:(h + 1) * qn]


def block_grads(i, j, **refs):
    rows = refs['raw'].shape[1]
    for q0 in (0, rows // 2):
        tile_grads(i, j, q0, rows // 2, rows, False, **refs)


def diagonal_grads(i, **refs):
    half = refs['raw'].shape[1] // 2
    tile_grads(i, i, 0, half, half, True, **refs)
    tile_grads(i, i, half, half, 2 * half, True, **refs)


def finish_q(c, raw, qw, tabs, dqt, dw):
    cos_t, sin_s = chunk_angles(c, *tabs)
    rows = raw.shape[1]
    for h in range(2):
        cols = slice(h * 128, (h + 1) * 128)
        grad = dqt[c, :, h * rows:(h + 1) * rows].T * SM_SCALE
        dx, part = norm_rope_grad(raw[c, :, cols].astype(F32), qw[...], cos_t, sin_s, grad)
        raw[c, :, cols] = dx.astype(BF16)
        dw[0:8, :] += part


def finish_k(c, raw, kw, tabs, dkt, dvt, dw):
    cos_t, sin_s = chunk_angles(c, *tabs)
    dx, part = norm_rope_grad(raw[c, :, 256:384].astype(F32), kw[...], cos_t, sin_s, dkt[c].T * SM_SCALE)
    raw[c, :, 256:384] = dx.astype(BF16)
    dw[8:16, :] += part
    raw[c, :, 384:512] = dvt[c].T.astype(BF16)


MESH = pl.DeviceIdType.MESH
EARLY = 5


def partner(me, step):
    total = me + step
    for bit in (1, 2, 4):
        total = total - 2 * bit * lax.rem(lax.div(me, bit), 2) * lax.rem(lax.div(step, bit), 2)
    return total


def visit_order(u):
    return u + 2 * lax.div(u, 4) * (1 - 2 * lax.rem(lax.div(u, 2), 2))


def attn_kernel(slab, ld_in, qw, kw, cos_o, sin_o, cos_c, sin_c, out, dw_out,
                raw, ld, qr, qt, dot_, kt, ext, dqt, dkt, dvt, dw, dw_all,
                send_in, recv_in, send_ld, recv_ld, send_out, recv_out, send_dw, recv_dw, own_sem):
    n_chunks = raw.shape[0]
    n_dev = n_chunks // 2
    me = lax.axis_index('cp')
    tabs = (cos_o, sin_o, cos_c, sin_c)
    refs = dict(raw=raw, qr=qr, qt=qt, dot_=dot_, kt=kt, ext=ext, dqt=dqt, dkt=dkt, dvt=dvt)
    block = functools.partial(block_grads, **refs)
    diagonal = functools.partial(diagonal_grads, **refs)

    def chunk_of(dev, half):
        return dev + half * (n_chunks - 1 - 2 * dev)

    def source(u):
        return partner(me, visit_order(jnp.int32(u)))

    def in_copy(half, dest, src):
        return pltpu.make_async_remote_copy(
            src_ref=slab.at[dest, half], dst_ref=raw.at[chunk_of(src, half)],
            send_sem=send_in.at[dest, half], recv_sem=recv_in.at[src, half],
            device_id={'cp': dest}, device_id_type=MESH)

    def ld_copy(dest, src):
        return pltpu.make_async_remote_copy(
            src_ref=ld_in.at[dest], dst_ref=ld.at[src],
            send_sem=send_ld.at[dest], recv_sem=recv_ld.at[src],
            device_id={'cp': dest}, device_id_type=MESH)

    def out_parts(part, half, chunk, src):
        cols = (pl.ds(0, 256), pl.ds(256, 256), pl.ds(0, 512))[part]
        return raw.at[chunk, :, cols], out.at[src, half, :, cols]

    def out_copy(part, half, dest, src, chunk):
        a, b = out_parts(part, half, chunk, src)
        return pltpu.make_async_remote_copy(
            src_ref=a, dst_ref=b, send_sem=send_out.at[dest, part], recv_sem=recv_out.at[src, part],
            device_id={'cp': dest}, device_id_type=MESH)

    def own_out(part, half):
        a, b = out_parts(part, half, chunk_of(me, half), me)
        return pltpu.make_async_copy(a, b, own_sem.at[3 + part])

    def dw_copy(dest, src):
        return pltpu.make_async_remote_copy(
            src_ref=dw, dst_ref=dw_all.at[src], send_sem=send_dw.at[dest], recv_sem=recv_dw.at[src],
            device_id={'cp': dest}, device_id_type=MESH)

    def loop(lo, hi, body):
        lax.fori_loop(lo, hi, lambda u, _: (body(u), 0)[1], 0)

    def loop_by_two(lo, hi, body):
        count = hi - lo

        def two(m):
            body(lo + 2 * m)
            body(lo + 2 * m + 1)

        loop(0, count // 2, two)

        @pl.when(count % 2 == 1)
        def _():
            body(hi - 1)

    own = [pltpu.make_async_copy(slab.at[me, h], raw.at[chunk_of(me, h)], own_sem.at[h]) for h in range(2)]
    own.append(pltpu.make_async_copy(ld_in.at[me], ld.at[me], own_sem.at[2]))
    for copy in own:
        copy.start()

    barrier = pltpu.get_barrier_semaphore()
    loop(1, n_dev, lambda u: pl.semaphore_signal(barrier, inc=1, device_id={'cp': source(u)}, device_id_type=MESH))
    pl.semaphore_wait(barrier, n_dev - 1)

    loop(1, n_dev, lambda u: ld_copy(source(u), me).start())
    for half in range(2):
        in_copy(half, source(1), me).start()
    loop(2, n_dev, lambda u: in_copy(0, source(u), me).start())

    dw[...] = jnp.zeros_like(dw)
    dqt[...] = jnp.zeros_like(dqt)
    dkt[...] = jnp.zeros_like(dkt)
    dvt[...] = jnp.zeros_like(dvt)
    for copy in own:
        copy.wait()

    def arrive(t):
        visit, half = stop(t)
        src = source(visit)

        @pl.when(visit > 0)
        def _():
            in_copy(half, me, src).wait_recv()

        @pl.when((visit > 0) & (half == 0))
        def _():
            ld_copy(me, src).wait_recv()

        @pl.when((t >= 4) & (t < 7))
        def _():
            for step in range(2):
                in_copy(1, source(2 * t - 6 + step), me).start()

        prep_chunk(chunk_of(src, half), src, half, raw, ld, qw, kw, tabs, qr, qt, dot_, kt, ext)

    def send(u, part, half):
        dest = source(u)

        @pl.when(u > 0)
        def _():
            out_copy(part, half, dest, me, chunk_of(dest, half)).start()

        @pl.when(u == 0)
        def _():
            own_out(part, half).start()

    def stop(t):
        t = jnp.int32(t)
        late = lax.div(t + 12, 16)
        visit = (1 - late) * lax.rem(t, 2) + late * (2 + lax.rem(t + 2, 6))
        half = (1 - late) * lax.div(t, 2) + late * (lax.div(t + 2, 6) - 1)
        return visit, half

    def chunk_at(t):
        visit, half = stop(t)
        return chunk_of(source(visit), half)

    def pair(a, b):
        block(jnp.maximum(a, b), jnp.minimum(a, b))

    def row_round(t):
        arrive(t)
        a = chunk_at(t)
        loop_by_two(0, t, lambda w: pair(a, chunk_at(w)))
        diagonal(a)

    n_low = n_dev + 2
    n_row = n_low + EARLY - 2
    loop(0, n_low, row_round)
    loop(n_low, n_row, row_round)
    loop(n_row, n_chunks, arrive)

    def low_queries(u):
        finish_q(source(u), raw, qw, tabs, dqt, dw)
        send(u, 0, 0)

    loop(0, n_dev, low_queries)

    def low_column(u):
        j = source(u)
        for w in range(n_row, n_chunks):
            block(chunk_at(w), j)
        finish_k(j, raw, kw, tabs, dkt, dvt, dw)
        send(u, 1, 0)

    loop(0, n_dev, low_column)

    def high_finish(u):
        a = chunk_of(source(u), 1)
        loop_by_two(jnp.maximum(u + 1, EARLY), n_dev, lambda w: pair(a, chunk_of(source(w), 1)))

        @pl.when(u >= EARLY)
        def _():
            diagonal(a)

        finish_q(a, raw, qw, tabs, dqt, dw)
        finish_k(a, raw, kw, tabs, dkt, dvt, dw)
        send(u, 2, 1)

    loop(0, n_dev, high_finish)

    loop(1, n_dev, lambda u: dw_copy(source(u), me).start())
    dw_all[me] = dw[...]

    def settle(u):
        src = source(u)
        ld_copy(src, me).wait_send()
        for half in range(2):
            in_copy(half, src, me).wait_send()
        for part in range(3):
            out_copy(part, part // 2, src, me, chunk_of(src, part // 2)).wait_send()
            out_copy(part, part // 2, me, src, chunk_of(me, part // 2)).wait_recv()
        dw_copy(src, me).wait_send()
        dw_copy(me, src).wait_recv()

    loop(1, n_dev, settle)
    for part in range(3):
        own_out(part, part // 2).wait()
    total = dw_all[0]
    for src in range(1, n_dev):
        total = total + dw_all[src]
    dw_out[...] = total


def run_attention(slab, ld, q_norm, k_norm, tabs):
    n_dev, _, rows, _ = slab.shape
    n_chunks = 2 * n_dev
    any_spec = pl.BlockSpec(memory_space=pl.ANY)
    vmem_spec = pl.BlockSpec(memory_space=pltpu.VMEM)
    dma = pltpu.SemaphoreType.DMA
    return pl.pallas_call(
        attn_kernel,
        out_shape=(jax.ShapeDtypeStruct((n_dev, 2, rows, 512), BF16), jax.ShapeDtypeStruct((16, HEAD_DIM), F32)),
        in_specs=[any_spec, any_spec] + [vmem_spec] * 6,
        out_specs=(any_spec, vmem_spec),
        scratch_shapes=[
            pltpu.VMEM((n_chunks, rows, 768), BF16),
            pltpu.VMEM((n_dev, 2, 8, rows), F32),
            pltpu.VMEM((n_chunks, rows, 384), BF16),
            pltpu.VMEM((n_chunks, HEAD_DIM, 2 * rows), BF16),
            pltpu.VMEM((n_chunks, HEAD_DIM, 2 * rows), BF16),
            pltpu.VMEM((n_chunks, HEAD_DIM, rows), BF16),
            pltpu.VMEM((n_chunks, rows, 256), BF16),
            pltpu.VMEM((n_chunks, HEAD_DIM, 2 * rows), F32),
            pltpu.VMEM((n_chunks, HEAD_DIM, rows), F32),
            pltpu.VMEM((n_chunks, HEAD_DIM, rows), F32),
            pltpu.VMEM((16, HEAD_DIM), F32),
            pltpu.VMEM((n_dev, 16, HEAD_DIM), F32),
            dma((n_dev, 2)), dma((n_dev, 2)), dma((n_dev,)), dma((n_dev,)),
            dma((n_dev, 3)), dma((n_dev, 3)), dma((n_dev,)), dma((n_dev,)), dma((6,)),
        ],
        compiler_params=pltpu.CompilerParams(vmem_limit_bytes=67043328, collective_id=0, has_side_effects=True),
        name='attention_backward',
    )(slab, ld, q_norm, k_norm, *tabs)


def pack_kernel(q, k, v, o, lse, do, slab, ld, wide):
    rows, heads = q.shape[0], q.shape[1]
    groups = k.shape[1]

    def scatter(x, n_heads, col):
        per = n_heads // groups
        wide[0:rows * n_heads, :] = x[...].reshape(rows * n_heads, HEAD_DIM).astype(F32)
        for h in range(n_heads):
            first = col + (h % per) * HEAD_DIM
            slab[h // per, :, first:first + HEAD_DIM] = wide[pl.ds(h, rows, stride=n_heads), :].astype(BF16)

    scatter(q, heads, 0)
    scatter(k, groups, 256)
    scatter(v, groups, 384)
    scatter(do, heads, 512)
    lse_t = lse[...].T
    delta_t = jnp.sum(do[...].astype(F32) * o[...].astype(F32), axis=-1).T
    for g in range(groups):
        ld[g, 0] = jnp.concatenate([lse_t[2 * g:2 * g + 2], delta_t[2 * g:2 * g + 2], jnp.zeros((4, rows), F32)], axis=0)


def pack_inputs(q, k, v, o, lse, do):
    local_rows, heads, _ = q.shape
    groups = k.shape[1]
    blk = min(128, local_rows // 2)
    per_half = local_rows // 2 // blk
    big = pl.BlockSpec((blk, heads, HEAD_DIM), lambda i: (i, 0, 0))
    small = pl.BlockSpec((blk, groups, HEAD_DIM), lambda i: (i, 0, 0))
    return pl.pallas_call(
        pack_kernel,
        grid=(local_rows // blk,),
        in_specs=[big, small, small, big, pl.BlockSpec((blk, heads), lambda i: (i, 0)), big],
        out_specs=(pl.BlockSpec((groups, blk, 768), lambda i: (0, i, 0)),
                   pl.BlockSpec((groups, 1, 8, blk), lambda i: (0, i // per_half, 0, i % per_half))),
        out_shape=(jax.ShapeDtypeStruct((groups, local_rows, 768), BF16),
                   jax.ShapeDtypeStruct((groups, 2, 8, local_rows // 2), F32)),
        scratch_shapes=[pltpu.VMEM((blk * heads, HEAD_DIM), F32)],
        name='pack_inputs',
    )(q, k, v, o, lse, do)


def unpack_kernel(out, dq, dk, dv, wide):
    rows, heads = dq.shape[0], dq.shape[1]
    groups = dk.shape[1]

    def gather(dst, n_heads, col):
        per = n_heads // groups
        for h in range(n_heads):
            first = col + (h % per) * HEAD_DIM
            wide[pl.ds(h, rows, stride=n_heads), :] = out[h // per, :, first:first + HEAD_DIM].astype(F32)
        dst[...] = wide[0:rows * n_heads, :].astype(BF16).reshape(rows, n_heads, HEAD_DIM)

    gather(dq, heads, 0)
    gather(dk, groups, 256)
    gather(dv, groups, 384)


def unpack_outputs(out, heads):
    groups, local_rows, _ = out.shape
    blk = min(128, local_rows // 2)
    big = pl.BlockSpec((blk, heads, HEAD_DIM), lambda i: (i, 0, 0))
    small = pl.BlockSpec((blk, groups, HEAD_DIM), lambda i: (i, 0, 0))
    return pl.pallas_call(
        unpack_kernel,
        grid=(local_rows // blk,),
        in_specs=[pl.BlockSpec((groups, blk, 512), lambda i: (0, i, 0))],
        out_specs=(big, small, small),
        out_shape=(jax.ShapeDtypeStruct((local_rows, heads, HEAD_DIM), BF16),
                   jax.ShapeDtypeStruct((local_rows, groups, HEAD_DIM), BF16),
                   jax.ShapeDtypeStruct((local_rows, groups, HEAD_DIM), BF16)),
        scratch_shapes=[pltpu.VMEM((blk * heads, HEAD_DIM), F32)],
        name='unpack_outputs',
    )(out)


def solution(mesh):
    cp_size = mesh.shape['cp']

    def local_grads(q_raw, k_raw, v_proj, out_fwd, lse_fwd, d_out, q_norm, k_norm):
        local_rows, num_heads = q_raw.shape[0], q_raw.shape[1]
        rows = local_rows // 2
        tabs = angle_tables(jnp.arange(rows)) + angle_tables(jnp.arange(2 * cp_size) * rows)
        slab, ld = pack_inputs(q_raw, k_raw, v_proj, out_fwd, lse_fwd, d_out)
        out, dw = run_attention(slab.reshape(cp_size, 2, rows, 768), ld, q_norm.reshape(1, -1), k_norm.reshape(1, -1), tabs)
        dq_raw, dk_raw, dv = unpack_outputs(out.reshape(cp_size, local_rows, 512), num_heads)
        return dq_raw, dk_raw, dv, dw[:8].sum(0), dw[8:].sum(0)

    row_spec = P(('dp', 'cp'))
    in_specs = (row_spec, row_spec, row_spec, row_spec, row_spec, row_spec, P(), P())
    out_specs = (row_spec, row_spec, row_spec, P('dp'), P('dp'))
    return jax.shard_map(local_grads, mesh=mesh, in_specs=in_specs, out_specs=out_specs, check_vma=False)
```
